32 devices in a mesh: expert: 4 (over x, core), replica: 8 (over z, y).
Axes of the slice: x: 2, y: 2, z: 4, core: 2. Of those that a mesh axis runs over, the one named last changes fastest.
Arguments:
- tokens: bfloat16 [8, 1024, 2048], P('replica', 'expert'), may hold values from -6 to 6
- out_grad: bfloat16 [8, 1024, 2048], P('replica', 'expert'), may hold values from -6 to 6
- routes: int32 [8, 1024, 2], P('replica', 'expert'), may hold values from 0 to 3, all different within a row; in each aligned block of 256 rows (0 to 255, 256 to 511, ..., all dimensions but the last counted through in order) at most 256 rows name the same one
- route_weight: bfloat16 [8, 1024, 2], P('replica', 'expert'), may hold values from 0.19921875 to 1
- gate_up_matrix: bfloat16 [8, 4, 2048, 512], P('replica', 'expert'), may hold values from -6 to 6
- down_matrix: bfloat16 [8, 4, 2048, 256], P('replica', 'expert'), may hold values from -6 to 6
- gate_up_velocity: bfloat16 [8, 4, 2048, 512], P('replica', 'expert'), may hold values from -6 to 6
- down_velocity: bfloat16 [8, 4, 2048, 256], P('replica', 'expert'), may hold values from -6 to 6
- partner: int32 [8], replicated, may hold values from 0 to 7, as said below
Outputs:
- token_grad: bfloat16 [8, 1024, 2048], P('replica', 'expert')
- mixed_gate_up: bfloat16 [8, 4, 2048, 512], P('replica', 'expert')
- mixed_down: bfloat16 [8, 4, 2048, 256], P('replica', 'expert')
The draws below stay inside these ranges and needn't reach their ends.
Inputs may be any that keep to these rules, and one draw needn't show every extreme that they name: `routes`: the rows of one device route at most 256 pairs to any one expert; no row names an expert twice. partner[r] = r xor s for one power of two s below 8, the same s for all r, so replicas are matched in pairs.
All inputs are finite; a program needn't handle non-finite values.
Results may differ from the reference program's by a relative error of at most 0.0065.
Values may be sent and summed in bfloat16 or wider, within the bound.
No kernel may reach another device: no remote copies, remote signals or barrier semaphores. Data moves between devices by JAX's collectives and lax.ppermute only.
A program may use at most 128 MiB of HBM per device.

```python
import math
import jax
import jax.numpy as jnp
import numpy as np
from jax import lax

MODEL_WIDTH = 2048
FF = 256
TOP = 2
TOK_DEV = 256
EXPERT_TOTAL = 4
REPLICAS = 8
CAP = 256
ROWS = 1024
N_EXPERT = 4


def draw_partner(key, part):
    levels = REPLICAS.bit_length() - 1
    level = jax.random.randint(jax.random.fold_in(key, 17), (), 0, levels, dtype=jnp.int32)
    offset = jnp.left_shift(jnp.ones((), jnp.int32), level)
    return jnp.bitwise_xor(jnp.arange(REPLICAS, dtype=jnp.int32), offset).astype(jnp.int32)


def block_levels(own_key, extent, cuts, smallest, high):
    def one(axis_at, parts):
        steps = jax.random.uniform(jax.random.fold_in(jax.random.fold_in(own_key, 6), axis_at), (parts,), jnp.float32, smallest / len(cuts), high / len(cuts))
        return jnp.repeat(jnp.exp(steps), extent[axis_at] // parts).reshape((-1,) + (1,) * (len(extent) - axis_at - 1))

    factor_of = one(*cuts[0])
    for cut in cuts[1:]:
        factor_of = factor_of * one(*cut)
    return factor_of


def assign_block(rng, own, number, rows, number_of, top, most, lean):
    order = jax.random.permutation(rng, number_of)
    heavy_load, common = portions_of(number_of, rows * top, most, lean, True), portions_of(number_of, rows * top, most, lean, False)
    places = jnp.arange(number_of)

    def named(sizes, rotation):
        used = int((sizes > 0).sum())
        fixed = max(1, used // 4)
        shifted = fixed + (places - fixed + rotation * (used - fixed)) % max(1, number_of - fixed)
        return jnp.zeros((number_of,), jnp.int32).at[order[jnp.where(places < fixed, places, shifted)]].set(jnp.asarray(sizes, jnp.int32))

    sizes = jnp.where(number % 4 == 0, named(heavy_load, number // 4), named(common, number - number // 4 - 1))
    mixed = jax.random.permutation(jax.random.fold_in(own, 3), number_of)
    giver, taker = mixed[0:number_of // 2 * 2:2], mixed[1:number_of // 2 * 2:2]
    margin = jnp.minimum(sizes[giver] - 1, most - sizes[taker]) // 2
    margin = jnp.where((giver == order[0]) | (taker == order[0]) | (sizes[taker] == 0), 0, jnp.maximum(margin, 0))
    shifted = jax.random.randint(jax.random.fold_in(own, 4), (number_of // 2,), 0, 1 << 20) % (margin + 1)
    sizes = sizes.at[giver].add(-shifted).at[taker].add(shifted)
    items = jnp.searchsorted(jnp.cumsum(sizes), jnp.arange(rows * top), side="right").astype(jnp.int32)
    listing = items.reshape(top, rows).T
    listing = listing[jax.random.permutation(jax.random.fold_in(own, 1), rows)]
    rotation = jax.random.randint(jax.random.fold_in(own, 2), (rows, 1), 0, top)
    return jnp.take_along_axis(listing, (jnp.arange(top)[None, :] + rotation) % top, axis=1)


def portions_of(number_of, total, most, skew, full):
    loads = [(1 << 20) // math.isqrt(grade ** skew) + 1 for grade in range(1, number_of + 1)]
    largest = most if full else min(most, max(-(-total // number_of), total * loads[0] // sum(loads)))
    least = 1 if total - largest >= number_of - 1 else 0
    holding, rest = [largest] + [least] * (number_of - 1), total - largest - least * (number_of - 1)
    while rest > 0:
        candidates = [i for i in range(1, number_of) if holding[i] < largest] or [i for i in range(1, number_of) if holding[i] < most]
        whole, left = sum([loads[i] for i in candidates]), rest
        for i in candidates:
            addition = min(most - holding[i], max(1, left * loads[i] // whole), rest)
            holding[i] = holding[i] + addition
            rest = rest - addition
    return np.array(holding)


def noise(own_key, dims, spread, most, cuts=(), kind=jnp.bfloat16):
    entries = spread * jax.random.normal(own_key, dims, jnp.float32)
    if cuts:
        entries = entries * block_levels(own_key, dims, cuts, -0.22, 0.18)
    return jnp.clip(entries, -most, most).astype(kind)


def setup_inputs(seed: int = 0) -> dict:
    splits = jax.random.split(jax.random.key(seed), 10)
    tokens = noise(splits[0], (REPLICAS, ROWS, MODEL_WIDTH), 1.0, 6.0, ((0, 8), (1, 4)))
    out_grad = noise(splits[1], (REPLICAS, ROWS, MODEL_WIDTH), 1.0, 6.0, ((0, 8), (1, 4)))
    routes_keys = jax.random.split(jax.random.fold_in(splits[2], 1), REPLICAS * ROWS // TOK_DEV)
    routes_turns = jax.random.permutation(jax.random.fold_in(splits[2], 3), REPLICAS * ROWS // TOK_DEV)
    routes = jax.vmap(lambda own, number: assign_block(jax.random.fold_in(splits[2], 2), own, number, TOK_DEV, EXPERT_TOTAL, TOP, CAP, 1))(routes_keys, routes_turns).reshape((REPLICAS, ROWS, TOP))
    route_weight = jnp.clip(0.19921875 + 0.80078125 * jax.random.uniform(splits[3], (REPLICAS, ROWS, TOP), jnp.float32) ** block_levels(splits[3], (REPLICAS, ROWS, TOP), ((0, 8), (1, 4)), -0.2, 0.2), 0.19921875, 1.0).astype(jnp.bfloat16)
    gate_up_matrix = noise(splits[4], (REPLICAS, EXPERT_TOTAL, MODEL_WIDTH, 2 * FF), 1.0, 6.0, ((0, 8), (1, 4)))
    down_matrix = noise(splits[5], (REPLICAS, EXPERT_TOTAL, MODEL_WIDTH, FF), 1.0, 6.0, ((0, 8), (1, 4)))
    gate_up_velocity = noise(splits[6], (REPLICAS, EXPERT_TOTAL, MODEL_WIDTH, 2 * FF), 1.0, 6.0, ((0, 8), (1, 4)))
    down_velocity = noise(splits[7], (REPLICAS, EXPERT_TOTAL, MODEL_WIDTH, FF), 1.0, 6.0, ((0, 8), (1, 4)))
    partner = draw_partner(jax.random.fold_in(splits[9], 71), 0)
    return {"tokens": tokens, "out_grad": out_grad, "routes": routes, "route_weight": route_weight, "gate_up_matrix": gate_up_matrix, "down_matrix": down_matrix, "gate_up_velocity": gate_up_velocity, "down_velocity": down_velocity, "partner": partner}


step_size = 0.2
momentum_decay = 0.9

def expert_gradient_pass(input_rows):
    input_buffer, gradient_buffer, gate_up_matrix, down_matrix, gate_up_velocity, down_velocity = input_rows
    inv_width = 1.0 / math.sqrt(MODEL_WIDTH)
    inverse_hidden = 1.0 / math.sqrt(FF)
    pre = jnp.dot(input_buffer, gate_up_matrix, preferred_element_type=jnp.float32) * inv_width
    gate = pre[:, :FF]
    up = pre[:, FF:]
    active = jax.nn.silu(gate)
    hidden_state = (active * up).astype(jnp.bfloat16)
    hidden_gradient = jnp.dot(gradient_buffer, down_matrix, preferred_element_type=jnp.float32) * inverse_hidden
    sigmoid_gate = jax.nn.sigmoid(gate)
    slope = sigmoid_gate * (1.0 + gate * (1.0 - sigmoid_gate))
    pre_grad = jnp.concatenate([hidden_gradient * up * slope, hidden_gradient * active], axis=1).astype(jnp.bfloat16)
    down_gradient = jnp.dot(gradient_buffer.T, hidden_state, preferred_element_type=jnp.float32) * inverse_hidden
    gate_up_grad = jnp.dot(input_buffer.T, pre_grad, preferred_element_type=jnp.float32) * inv_width
    paired_gradient = (jnp.dot(pre_grad, gate_up_matrix.T, preferred_element_type=jnp.float32) * inv_width).astype(jnp.bfloat16)
    next_gate_up = (gate_up_matrix.astype(jnp.float32) - step_size * (momentum_decay * gate_up_velocity.astype(jnp.float32) + gate_up_grad)).astype(jnp.bfloat16)
    next_down_matrix = (down_matrix.astype(jnp.float32) - step_size * (momentum_decay * down_velocity.astype(jnp.float32) + down_gradient)).astype(jnp.bfloat16)
    return (paired_gradient, next_gate_up, next_down_matrix)

def one_replica(input_rows):
    tokens, out_grad, routes, route_weight, gate_up_matrix, down_matrix, gate_up_velocity, down_velocity = input_rows
    buffered_rows = N_EXPERT * CAP
    flat_ids = routes.reshape(-1).astype(jnp.int32)
    pairs = flat_ids.shape[0]
    token_of = (jnp.arange(pairs, dtype=jnp.int32) // TOP).astype(jnp.int32)
    onehot = (flat_ids[:, None] == jnp.arange(EXPERT_TOTAL, dtype=jnp.int32)[None, :]).astype(jnp.int32)
    ranks = lax.optimization_barrier(jnp.sum((jnp.cumsum(onehot, axis=0) - onehot) * onehot, axis=1)).astype(jnp.int32)
    slot_lookup = (flat_ids * buffered_rows + ranks).astype(jnp.int32)
    row_inputs = tokens[token_of]
    scaled_rows = (out_grad[token_of].astype(jnp.float32) * route_weight.reshape(-1)[:, None].astype(jnp.float32)).astype(jnp.bfloat16)
    input_buffer = jnp.zeros((EXPERT_TOTAL * buffered_rows, MODEL_WIDTH), jnp.bfloat16).at[slot_lookup].set(row_inputs)
    gradient_buffer = jnp.zeros((EXPERT_TOTAL * buffered_rows, MODEL_WIDTH), jnp.bfloat16).at[slot_lookup].set(scaled_rows)
    paired_gradient, next_gate_up, next_down_matrix = lax.map(expert_gradient_pass, (input_buffer.reshape(EXPERT_TOTAL, buffered_rows, MODEL_WIDTH), gradient_buffer.reshape(EXPERT_TOTAL, buffered_rows, MODEL_WIDTH), gate_up_matrix, down_matrix, gate_up_velocity, down_velocity))
    gathered = paired_gradient.reshape(EXPERT_TOTAL * buffered_rows, MODEL_WIDTH)[slot_lookup]
    token_grad = lax.optimization_barrier(jnp.sum(gathered.astype(jnp.float32).reshape(-1, TOP, MODEL_WIDTH), axis=1)).astype(jnp.bfloat16)
    return (token_grad, next_gate_up, next_down_matrix)

def mix_pair(input_rows):
    own_weight, other_weight = input_rows
    return (0.5 * (own_weight.astype(jnp.float32) + other_weight.astype(jnp.float32))).astype(jnp.bfloat16)

def reference(tokens, out_grad, routes, route_weight, gate_up_matrix, down_matrix, gate_up_velocity, down_velocity, partner):
    token_grad, next_gate_up, next_down_matrix = lax.map(one_replica, (tokens, out_grad, routes, route_weight, gate_up_matrix, down_matrix, gate_up_velocity, down_velocity))
    mixed_gate_up = lax.map(mix_pair, (next_gate_up, next_gate_up[partner]))
    mixed_down = lax.map(mix_pair, (next_down_matrix, next_down_matrix[partner]))
    return (token_grad, mixed_gate_up, mixed_down)
```

```python
import functools
import math

import jax
import jax.numpy as jnp
from jax import lax
from jax.experimental import pallas as pl
from jax.experimental.pallas import tpu as pltpu
from jax.sharding import PartitionSpec as P


step_size = 0.2
momentum_decay = 0.9


def shortened(value):

    def short(part):
        return part.astype(jnp.bfloat16) if part.dtype == jnp.float32 else part

    return jax.tree.map(short, value)


def partner_2(block, axis, bit):
    count = lax.axis_size(axis)
    route = []
    for low in range(count):
        high = low | 1 << bit
        if high != low and high < count:
            route += [(low, high), (high, low)]
    return lax.ppermute(block, axis, route)


def contract_leading(left, right):
    return lax.dot_general(
        left, right, (((0,), (0,)), ((), ())), preferred_element_type=jnp.float32
    )


def swap_level(value, level):
    return jax.tree.map(
        lambda part, own: part.astype(own.dtype),
        partner_2(shortened(value), "replica", level),
        value,
    )


def routed_layer(
    tokens,
    out_grad,
    routes,
    route_weight,
    gate_up_matrix,
    down_matrix,
    gate_up_velocity,
    down_velocity,
    partner,
):
    expert_count = lax.axis_size("expert")
    tok_rows = tokens.shape[1]
    top_count = routes.shape[2]
    feature_width = tokens.shape[2]
    hidden_width = down_matrix.shape[3]
    capacity = 2 * tok_rows * top_count // expert_count
    slot_total = expert_count * capacity
    inv_width = 1.0 / math.sqrt(feature_width)
    inverse_hidden = 1.0 / math.sqrt(hidden_width)
    flat_ids = routes[0].reshape(-1)
    onehot = (flat_ids[:, None] == jnp.arange(expert_count, dtype=jnp.int32)[None, :]).astype(
        jnp.int32
    )
    ranks = jnp.sum((jnp.cumsum(onehot, axis=0) - onehot) * onehot, axis=1)
    slot_lookup = flat_ids * capacity + ranks
    chosen = (slot_lookup[None, :] == jnp.arange(slot_total, dtype=jnp.int32)[:, None]).reshape(
        slot_total, tok_rows, top_count
    )
    picker = jnp.any(chosen, axis=2).astype(jnp.bfloat16)
    weighted = jnp.sum(
        jnp.where(chosen, route_weight[0][None, :, :], jnp.zeros((), jnp.bfloat16)), axis=2
    )
    sent_inputs = jnp.dot(picker, tokens[0], preferred_element_type=jnp.float32).astype(
        jnp.bfloat16
    )
    sent_grads = jnp.dot(weighted, out_grad[0], preferred_element_type=jnp.float32).astype(
        jnp.bfloat16
    )
    recv_inputs, received_gradients = (
        lax.all_to_all(
            sent_inputs.reshape(expert_count, capacity, feature_width),
            "expert",
            split_axis=0,
            concat_axis=0,
            tiled=True,
        ),
        lax.all_to_all(
            sent_grads.reshape(expert_count, capacity, feature_width),
            "expert",
            split_axis=0,
            concat_axis=0,
            tiled=True,
        ),
    )
    input_buffer = recv_inputs.reshape(slot_total, feature_width)
    gradient_buffer = received_gradients.reshape(slot_total, feature_width)
    weight_gu = gate_up_matrix[0, 0]
    down_projection_weight = down_matrix[0, 0]
    pre = jnp.dot(input_buffer, weight_gu, preferred_element_type=jnp.float32) * inv_width
    gate = pre[:, :hidden_width]
    upper = pre[:, hidden_width:]
    active = jax.nn.silu(gate)
    hidden_state = (active * upper).astype(jnp.bfloat16)
    hidden_gradient = (
        jnp.dot(gradient_buffer, down_projection_weight, preferred_element_type=jnp.float32)
        * inverse_hidden
    )
    sigmoid_gate = jax.nn.sigmoid(gate)
    slope = sigmoid_gate * (1.0 + gate * (1.0 - sigmoid_gate))
    pre_grad = jnp.concatenate(
        [hidden_gradient * upper * slope, hidden_gradient * active], axis=1
    ).astype(jnp.bfloat16)
    down_gradient = contract_leading(gradient_buffer, hidden_state) * inverse_hidden
    gate_up_grad = contract_leading(input_buffer, pre_grad) * inv_width
    new_gu = (
        weight_gu.astype(jnp.float32)
        - step_size * (momentum_decay * gate_up_velocity[0, 0].astype(jnp.float32) + gate_up_grad)
    ).astype(jnp.bfloat16)
    next_down_matrix = (
        down_projection_weight.astype(jnp.float32)
        - step_size * (momentum_decay * down_velocity[0, 0].astype(jnp.float32) + down_gradient)
    ).astype(jnp.bfloat16)
    new_gu, next_down_matrix = (new_gu, next_down_matrix)
    replica_count = lax.axis_size("replica")
    bit_total = replica_count.bit_length() - 1
    offset = jnp.bitwise_xor(partner[0], 0)
    level_index = jnp.zeros((), jnp.int32)
    for bit_index in range(bit_total):
        level_index = level_index + bit_index * jnp.bitwise_and(
            jnp.right_shift(offset, bit_index), 1
        )
    joined = jnp.concatenate([new_gu, next_down_matrix], axis=1)
    branches = [functools.partial(swap_level, level=level) for level in range(bit_total)]
    moved = lax.switch(level_index, branches, joined)
    mixed = (0.5 * (joined.astype(jnp.float32) + moved.astype(jnp.float32))).astype(jnp.bfloat16)
    mixed_gu = mixed[:, : 2 * hidden_width]
    mixed_dn = mixed[:, 2 * hidden_width :]
    paired_gradient = (
        lax.dot_general(
            pre_grad, weight_gu, (((1,), (1,)), ((), ())), preferred_element_type=jnp.float32
        )
        * inv_width
    ).astype(jnp.bfloat16)
    returned = lax.all_to_all(
        paired_gradient.reshape(expert_count, capacity, feature_width),
        "expert",
        split_axis=0,
        concat_axis=0,
        tiled=True,
    )
    combined = contract_leading(picker, returned.reshape(slot_total, feature_width))
    token_grad = combined.astype(jnp.bfloat16)[None]
    return (token_grad, mixed_gu[None, None], mixed_dn[None, None])


def swap(block, axis, bit):
    count = lax.axis_size(axis)
    return lax.ppermute(block, axis, [(i, i ^ (1 << bit)) for i in range(count)])


def call(body, outs, *args, grid=None, in_specs=None, out_specs=None, flops=0, aliases=None):
    size = sum(a.size * a.dtype.itemsize for a in args)
    size += sum(math.prod(o.shape) * o.dtype.itemsize for o in outs)
    options = {}
    if grid is not None:
        options = dict(grid=grid, in_specs=in_specs, out_specs=out_specs)
    return pl.pallas_call(
        body,
        out_shape=outs,
        input_output_aliases=aliases or {},
        compiler_params=pltpu.CompilerParams(vmem_limit_bytes=40 << 20),
        cost_estimate=pl.CostEstimate(flops=max(flops, size), bytes_accessed=size, transcendentals=0),
        **options,
    )(*args)


def shape(dims, dtype=jnp.bfloat16):
    return jax.ShapeDtypeStruct(dims, dtype)


def mm(left, right, dims=(1, 0)):
    return lax.dot_general(
        left, right, (((dims[0],), (dims[1],)), ((), ())), preferred_element_type=jnp.float32
    )


def split_body(count, wide, x_ref, *out_refs):
    for i in range(count):
        out_refs[i][...] = x_ref[:, i * wide : (i + 1) * wide]


def forward_body(scale, hidden, x_ref, w_ref, state_ref, first_ref, second_ref, turned_ref):
    x = x_ref[...]
    pre = mm(x, w_ref[...]) * scale
    gate, up = pre[:, :hidden], pre[:, hidden:]
    sig = jax.nn.sigmoid(gate)
    active = gate * sig
    state_ref[...] = (active * up).astype(jnp.bfloat16)
    first_ref[...] = up * (sig * (1.0 + gate * (1.0 - sig)))
    second_ref[...] = active
    turned_ref[...] = x.T


def scaled(me, grad, share):
    lane = lax.broadcasted_iota(jnp.int32, share.shape, 1)
    own = jnp.sum(jnp.where(lane == me, share.astype(jnp.float32), 0.0), axis=1, keepdims=True)
    return (grad.astype(jnp.float32) * own).astype(jnp.bfloat16)


def near_grad_body(me_ref, ga_ref, gb_ref, sa_ref, sb_ref, ha_ref, hb_ref, w_ref, d_ref, oa_ref, ob_ref):
    me = me_ref[0]
    w = w_ref[...]

    @pl.when(pl.program_id(0) == 0)
    def _():
        oa_ref[...] = jnp.zeros_like(oa_ref)
        ob_ref[...] = jnp.zeros_like(ob_ref)

    ga = scaled(me, ga_ref[...], sa_ref[...])
    gb = scaled(me, gb_ref[...], sb_ref[...])
    d_ref[...] = mm(ga, ha_ref[...], (0, 0)) + mm(gb, hb_ref[...], (0, 0))
    oa_ref[...] += mm(ga, w)
    ob_ref[...] += mm(gb, w)


def moved_weight(weight, speed, grad):
    value = weight.astype(jnp.float32) - step_size * (momentum_decay * speed.astype(jnp.float32) + grad)
    return value.astype(jnp.bfloat16)


def far_grad_body(
    scale, me_ref, gc_ref, gd_ref, sc_ref, sd_ref, hc_ref, hd_ref, w_ref, v_ref, d_ref, ic_ref, id_ref,
    u_ref, oc_ref, od_ref,
):
    me = me_ref[0]
    w = w_ref[...]
    gc = scaled(me, gc_ref[...], sc_ref[...])
    gd = scaled(me, gd_ref[...], sd_ref[...])
    d = d_ref[...] + mm(gc, hc_ref[...], (0, 0)) + mm(gd, hd_ref[...], (0, 0))
    u_ref[...] = moved_weight(w, v_ref[...], d * scale)
    oc_ref[...] = ic_ref[...] + mm(gc, w)
    od_ref[...] = id_ref[...] + mm(gd, w)


def pre_grad_of(scale, grad, first, second):
    grad = grad * scale
    return jnp.concatenate([(grad * first), (grad * second)], axis=1).astype(jnp.bfloat16)


def near_weight_body(scale, ga_ref, gb_ref, fa_ref, fb_ref, sa_ref, sb_ref, ta_ref, tb_ref, d_ref, pa_ref, pb_ref):
    @pl.when(pl.program_id(0) == 0)
    def _():
        pa_ref[...] = pre_grad_of(scale, ga_ref[...], fa_ref[...], sa_ref[...])
        pb_ref[...] = pre_grad_of(scale, gb_ref[...], fb_ref[...], sb_ref[...])

    d_ref[...] = mm(ta_ref[...], pa_ref[...]) + mm(tb_ref[...], pb_ref[...])


def far_pre_grad_body(scale, gc_ref, gd_ref, fc_ref, fd_ref, sc_ref, sd_ref, pc_ref, pd_ref):
    pc_ref[...] = pre_grad_of(scale, gc_ref[...], fc_ref[...], sc_ref[...])
    pd_ref[...] = pre_grad_of(scale, gd_ref[...], fd_ref[...], sd_ref[...])


def far_weight_body(scale, pc_ref, pd_ref, tc_ref, td_ref, d_ref, w_ref, v_ref, u_ref):
    d = d_ref[...] + mm(tc_ref[...], pc_ref[...]) + mm(td_ref[...], pd_ref[...])
    u_ref[...] = moved_weight(w_ref[...], v_ref[...], d * scale)


def back_body(scale, p_ref, w_ref, *refs):
    value = (mm(p_ref[...], w_ref[...], (1, 1)) * scale).astype(jnp.bfloat16)
    if len(refs) > 1:
        total = value.astype(jnp.float32)
        for ref in refs[:-1]:
            total = total + ref[...].astype(jnp.float32)
        value = total.astype(jnp.bfloat16)
    refs[-1][...] = value


def mix_body(own_ref, moved_ref, *refs):
    total = own_ref[...].astype(jnp.float32) + moved_ref[...].astype(jnp.float32)
    refs[-1][...] = (0.5 * total).astype(jnp.bfloat16)


def dense_layer(level, me, tokens, out_grad, shares, gate_up, down, gate_up_velocity, down_velocity):
    return dense_steps(
        level, me, tokens, out_grad, shares, gate_up, down, gate_up_velocity, down_velocity
    )


def dense_steps(level, me, tokens, out_grad, shares, gate_up, down, gate_up_velocity, down_velocity):
    grad_parts, weight_parts = GRAD_PARTS, WEIGHT_PARTS
    rows, width = tokens.shape
    hidden = down.shape[1]
    inv_width = 1.0 / math.sqrt(width)
    inv_hidden = 1.0 / math.sqrt(hidden)
    core, chip = 0, 1
    wide, high = width // grad_parts, width // weight_parts
    f32 = jnp.float32
    half = shape((rows, hidden), f32)
    scalar = pl.BlockSpec(memory_space=pltpu.SMEM)

    def whole(a):
        return pl.BlockSpec(a.shape, lambda i: (0,) * len(a.shape))

    chip_tokens = swap(tokens, "expert", chip)
    grads = call(
        functools.partial(split_body, grad_parts, wide),
        [shape((rows, wide))] * grad_parts, out_grad,
    )
    chip_grads = [swap(grads[i], "expert", chip) for i in range(grad_parts)]
    core_tokens = swap(tokens, "expert", core)
    core_shares = swap(shares, "expert", core)
    chip_shares = swap(shares, "expert", chip)
    core_grads = swap(out_grad, "expert", core)
    far_shares = swap(chip_shares, "expert", core)
    far_tokens = swap(chip_tokens, "expert", core)
    far_grads = [swap(g, "expert", core) for g in chip_grads]

    def forward(x):
        return call(
            functools.partial(forward_body, inv_width, hidden),
            [shape((rows, hidden)), half, half, shape((width, rows))], x, gate_up,
            flops=4 * rows * width * hidden,
        )

    ha, fa, sa, ta = forward(tokens)
    hb, fb, sb, tb = forward(core_tokens)
    col = pl.BlockSpec((rows, wide), lambda i: (0, i))
    row = pl.BlockSpec((wide, hidden), lambda i: (i, 0))
    near_down, ga, gb = call(
        near_grad_body, [shape((width, hidden), f32), half, half],
        me, out_grad, core_grads, shares, core_shares, ha, hb, down,
        grid=(grad_parts,),
        in_specs=[scalar, col, col, whole(shares), whole(shares), whole(ha), whole(hb), row],
        out_specs=[row, whole(half), whole(half)],
        flops=8 * rows * width * hidden,
    )
    tall = pl.BlockSpec((high, rows), lambda i: (i, 0))
    full = pl.BlockSpec((high, 2 * hidden), lambda i: (i, 0))
    pair = shape((rows, 2 * hidden))
    near_gu, pa, pb = call(
        functools.partial(near_weight_body, inv_hidden),
        [shape(gate_up.shape, f32), pair, pair], ga, gb, fa, fb, sa, sb, ta, tb,
        grid=(weight_parts,),
        in_specs=[whole(half)] * 6 + [tall, tall],
        out_specs=[full, whole(pair), whole(pair)],
        flops=8 * rows * width * hidden,
    )
    hc, fc, sc, tc = forward(chip_tokens)
    hd, fd, sd, td = forward(far_tokens)
    gc = gd = jnp.zeros(half.shape, f32)
    own_down, moved_down = [], []
    for i in range(grad_parts):
        part = pl.BlockSpec((wide, hidden), lambda _, i=i: (i, 0))
        u, gc, gd = call(
            functools.partial(far_grad_body, inv_hidden),
            [shape((wide, hidden)), half, half],
            me, chip_grads[i], far_grads[i], chip_shares, far_shares, hc, hd,
            down, down_velocity, near_down, gc, gd,
            grid=(1,),
            in_specs=[scalar, whole(grads[i]), whole(grads[i]), whole(shares), whole(shares),
                      whole(hc), whole(hd), part, part, part, whole(half), whole(half)],
            out_specs=[whole(shape((wide, hidden))), whole(half), whole(half)],
            flops=8 * rows * wide * hidden,
        )
        own_down.append(u)
        moved_down.append(swap(u, "replica", level))
    pc, pd = call(functools.partial(far_pre_grad_body, inv_hidden), [pair, pair], gc, gd, fc, fd, sc, sd)
    own_gu, moved_gu = [], []
    for i in range(weight_parts):
        part = pl.BlockSpec((high, 2 * hidden), lambda _, i=i: (i, 0))
        turned = pl.BlockSpec((high, rows), lambda _, i=i: (i, 0))
        u = call(
            functools.partial(far_weight_body, inv_width),
            [shape((high, 2 * hidden))], pc, pd, tc, td, near_gu, gate_up, gate_up_velocity,
            grid=(1,),
            in_specs=[whole(pair), whole(pair), turned, turned, part, part, part],
            out_specs=[whole(shape((high, 2 * hidden)))],
            flops=8 * rows * high * hidden,
        )[0]
        own_gu.append(u)
        moved_gu.append(swap(u, "replica", level))

    def back(p, *more):
        return call(
            functools.partial(back_body, inv_width), [shape((rows, width))], p, gate_up, *more,
            flops=4 * rows * width * hidden,
        )[0]

    for_far = swap(back(pd), "expert", core)
    for_core = swap(back(pb), "expert", core)
    for_chip = swap(back(pc, for_far), "expert", chip)
    token_grad = back(pa, for_core, for_chip)

    def mixed(own, moved, total):
        out = None
        for i, (a, b) in enumerate(zip(own, moved)):
            spot = pl.BlockSpec(a.shape, lambda _, i=i: (i, 0))
            args = (a, b) if out is None else (a, b, out)
            specs = [whole(a), whole(a)] + [pl.BlockSpec(memory_space=pl.ANY)] * (len(args) - 2)
            out = call(
                mix_body, [shape(total)], *args,
                grid=(1,), in_specs=specs, out_specs=[spot],
                aliases={2: 0} if out is not None else None,
            )[0]
        return out

    mixed_dn = mixed(own_down, moved_down, down.shape)
    mixed_gu = mixed(own_gu, moved_gu, gate_up.shape)
    return token_grad[None], mixed_gu[None, None], mixed_dn[None, None]


GRAD_PARTS, WEIGHT_PARTS = 4, 4


def per_device(
    tokens, out_grad, routes, route_weight, gate_up_matrix, down_matrix, gate_up_velocity, down_velocity, partner
):
    experts = lax.axis_size("expert")
    _, top_count = routes.shape[1:]
    if not dense(experts, top_count):
        return routed_layer(
            tokens, out_grad, routes, route_weight, gate_up_matrix, down_matrix, gate_up_velocity, down_velocity, partner
        )
    levels = lax.axis_size("replica").bit_length() - 1
    level = sum(
        bit * jnp.bitwise_and(jnp.right_shift(partner[0], bit), 1) for bit in range(levels)
    )
    named = routes[0][:, :, None] == jnp.arange(experts, dtype=jnp.int32)
    shares = jnp.sum(jnp.where(named, route_weight[0][:, :, None], jnp.zeros((), jnp.bfloat16)), axis=1)
    me = lax.axis_index("expert").reshape(1)
    branches = [functools.partial(dense_layer, i) for i in range(levels)]
    return lax.switch(
        level, branches, me, tokens[0], out_grad[0], shares, gate_up_matrix[0, 0], down_matrix[0, 0],
        gate_up_velocity[0, 0], down_velocity[0, 0],
    )


def dense(experts, top_count):
    return experts == 4 and 2 * top_count >= experts


def solution(mesh):
    placed = (
        P("replica", "expert", None),
        P("replica", "expert", None),
        P("replica", "expert", None),
        P("replica", "expert", None),
        P("replica", "expert", None, None),
        P("replica", "expert", None, None),
        P("replica", "expert", None, None),
        P("replica", "expert", None, None),
        P(),
    )
    return jax.shard_map(
        per_device,
        mesh=mesh,
        in_specs=placed,
        out_specs=(
            P("replica", "expert", None),
            P("replica", "expert", None, None),
            P("replica", "expert", None, None),
        ),
        check_vma=False,
    )
```
